512 devices in a mesh: grp: 16 (over y, core), blk: 32 (over z, x).
Axes of the slice: x: 4, y: 8, z: 8, core: 2. Of those that a mesh axis runs over, the one named last changes fastest.
Arguments:
- grads: bfloat16 [512, 4096, 128], P(('grp', 'blk')), may hold values from -6 to 6
- picks: int32 [512, 4096], P(('grp', 'blk')), may hold values from 0 to 511, as said below
- slot_map: int32 [512, 512], P(('grp', 'blk')), may hold values from 0 to 511, each once within a row
- momentum: float32 [262144, 128], P(('grp', 'blk')), may hold values from -6 to 6
- params: float32 [262144, 128], P(('grp', 'blk')), may hold values from -6 to 6
Outputs:
- new_momentum: float32 [262144, 128], P(('grp', 'blk'))
- new_params: float32 [262144, 128], P(('grp', 'blk'))
The draws below stay inside these ranges and needn't reach their ends.
Inputs may be any that keep to these rules, and one draw needn't show every extreme that they name: `picks`: for each replica and owner, the 8 entries in order: the j-th lies in [j * 64, (j + 1) * 64). `slot_map`: each row is a permutation of the 512 slots.
All inputs are finite; a program needn't handle non-finite values.
Results may differ from the reference program's by a relative error of at most 0.0003.
Values may be sent and summed in bfloat16 or wider, within the bound.
No kernel may reach another device: no remote copies, remote signals or barrier semaphores. Data moves between devices by JAX's collectives and lax.ppermute only.
A program may use at most 64 MiB of HBM per device.

```python
import jax
import jax.numpy as jnp
from jax import lax

BLOCK = 128
PICK = 8
OWN = 512
ITEMS = 4096
TOTAL = 262144
DEVICES = 512


def draw_picks(key, part):
    width = OWN // PICK
    offsets = jax.random.randint(key, (DEVICES, DEVICES, PICK), 0, width, dtype=jnp.int32)
    starts = jnp.arange(PICK, dtype=jnp.int32) * width
    return (offsets + starts[None, None, :]).reshape(DEVICES, DEVICES * PICK)


def steps_of(stream_key, shape, shards, low, top_value):
    def one(axis_at, shards_of):
        heights = jax.random.uniform(jax.random.fold_in(jax.random.fold_in(stream_key, 6), axis_at), (shards_of,), jnp.float32, low / len(shards), top_value / len(shards))
        return jnp.repeat(jnp.exp(heights), shape[axis_at] // shards_of).reshape((-1,) + (1,) * (len(shape) - axis_at - 1))

    gain = one(*shards[0])
    for cut in shards[1:]:
        gain = gain * one(*cut)
    return gain


def bell_draw(stream_key, shape, spread, bound, shards=(), kind=jnp.bfloat16):
    gain = steps_of(stream_key, shape, shards, -0.22, 0.18) if shards else 1.0
    values = jax.random.normal(stream_key, shape, jnp.float32) * spread * gain
    return jnp.minimum(jnp.maximum(values, -bound), bound).astype(kind)


def setup_inputs(seed: int = 0) -> dict:
    arg_keys = jax.random.split(jax.random.key(seed), 6)
    return {
        "grads": bell_draw(arg_keys[0], (DEVICES, ITEMS, BLOCK), 1.0, 6.0, ((0, 512),)),
        "picks": draw_picks(jax.random.fold_in(arg_keys[5], 71), 0),
        "slot_map": jax.vmap(lambda own: jax.random.permutation(own, OWN))(jax.random.split(arg_keys[2], DEVICES)).reshape((DEVICES, OWN)).astype(jnp.int32),
        "momentum": bell_draw(arg_keys[3], (TOTAL, BLOCK), 1.0, 6.0, ((0, 512),), jnp.float32),
        "params": bell_draw(arg_keys[4], (TOTAL, BLOCK), 1.0, 6.0, ((0, 512),), jnp.float32),
    }


def reference(grads, picks, slot_map, momentum, params):
    owners = slot_map.shape[0]
    owned = slot_map.shape[1]
    block = grads.shape[-1]
    owner_item = jnp.repeat(jnp.arange(owners, dtype=jnp.int32), PICK)

    def add_replica(total, inputs):
        values, chosen = inputs
        slots = slot_map[owner_item, chosen].astype(jnp.int32) + owner_item * owned
        return total.at[slots].add(values.astype(jnp.float32)), None

    start = jnp.zeros((owners * owned, block), jnp.float32)
    gradient, _ = lax.scan(add_replica, start, (grads, picks))
    new_momentum = 0.9 * momentum + gradient
    new_params = params - 0.05 * (gradient + 0.9 * new_momentum)
    return new_momentum, new_params
```

```python
import functools

import jax
import jax.numpy as jnp
from jax import lax
from jax.experimental import pallas as pl
from jax.experimental.pallas import tpu as pltpu
from jax.sharding import PartitionSpec as P

PAIR = 2
VMEM_LIMIT = 16 * 1024 * 1024


def pack(owners, tiles, window, grads_ref, picks_ref, out_ref, sem):
    copy = pltpu.make_async_copy(grads_ref, out_ref.at[:, 0:tiles], sem)
    copy.start()
    rows = picks_ref.shape[0]
    share = owners // rows
    offsets = lax.rem(picks_ref[...], window).astype(jnp.float32).astype(jnp.bfloat16)
    for r in range(rows):
        row = jnp.broadcast_to(offsets[r : r + 1][None], (share, PAIR, offsets.shape[1]))
        out_ref[r * share : (r + 1) * share, tiles] = row
    copy.wait()


def regroup(tiles, in_ref, out_ref, sems):
    copies = [pltpu.make_async_copy(in_ref.at[:, k], out_ref.at[k], sems.at[k]) for k in range(tiles + 1)]
    for copy in copies:
        copy.start()
    for copy in copies:
        copy.wait()


def update(
    pick, window, share, got_ref, slots_ref, mom_ref, par_ref, new_mom_ref, new_par_ref, numbers_ref
):
    tiles = pick // PAIR
    owned, block = mom_ref.shape
    count = got_ref.shape[1]
    numbers_ref[...] = got_ref[tiles].astype(jnp.float32).T
    first = lax.rem(lax.axis_index("blk"), share) * pick
    mine = numbers_ref[pl.ds(pl.multiple_of(first, pick), pick), :]
    lane = lax.broadcasted_iota(jnp.int32, (1, count), 1)
    odd = lax.rem(lane, PAIR) == 1
    place = lax.broadcasted_iota(jnp.int32, (PAIR * window, count), 0).astype(jnp.float32)
    parts = []
    for k in range(tiles):
        key = jnp.where(odd, mine[PAIR * k + 1 : PAIR * k + 2] + float(window), mine[PAIR * k : PAIR * k + 1])
        onehot = jnp.where(place == key, 1.0, 0.0).astype(jnp.bfloat16)
        parts.append(jnp.dot(onehot, got_ref[k], preferred_element_type=jnp.float32))
    merged = jnp.concatenate(parts, axis=0)
    high = merged.astype(jnp.bfloat16)
    rest = merged - high.astype(jnp.float32)
    middle = rest.astype(jnp.bfloat16)
    low = (rest - middle.astype(jnp.float32)).astype(jnp.bfloat16)
    slots = lax.broadcasted_iota(jnp.int32, (owned, owned), 0)
    placing = jnp.where(slots == slots_ref[...], 1.0, 0.0).astype(jnp.bfloat16)
    sums = jnp.dot(
        placing, jnp.concatenate([high, middle, low], axis=1), preferred_element_type=jnp.float32
    )
    gradient = sums[:, :block] + (sums[:, block : 2 * block] + sums[:, 2 * block :])
    new_momentum = 0.9 * mom_ref[...] + gradient
    new_mom_ref[...] = new_momentum
    new_par_ref[...] = par_ref[...] - 0.05 * (gradient + 0.9 * new_momentum)


def shards(grads, picks, slot_map, momentum, params):
    devices = lax.axis_size("grp") * lax.axis_size("blk")
    items, block = grads.shape[1:]
    owned = slot_map.shape[1]
    pick = items // devices
    tiles = pick // PAIR
    window = owned // pick
    rows = items // block
    vmem = pl.BlockSpec(memory_space=pltpu.VMEM)
    anywhere = pl.BlockSpec(memory_space=pl.ANY)
    distant = pl.BlockSpec(memory_space=pltpu.HBM)
    params_of = pltpu.CompilerParams(vmem_limit_bytes=VMEM_LIMIT)
    packed = pl.pallas_call(
        functools.partial(pack, devices, tiles, window),
        out_shape=jax.ShapeDtypeStruct((devices, tiles + 1, PAIR, block), grads.dtype),
        in_specs=[distant, vmem],
        out_specs=vmem,
        scratch_shapes=[pltpu.SemaphoreType.DMA],
        compiler_params=params_of,
        name="pack",
    )(grads.reshape(devices, tiles, PAIR, block), picks.reshape(rows, block))
    arrived = lax.all_to_all(packed, ("grp", "blk"), split_axis=0, concat_axis=0, tiled=True)
    grouped = pl.pallas_call(
        functools.partial(regroup, tiles),
        out_shape=jax.ShapeDtypeStruct((tiles + 1, devices, PAIR, block), grads.dtype),
        in_specs=[anywhere],
        out_specs=vmem,
        scratch_shapes=[pltpu.SemaphoreType.DMA((tiles + 1,))],
        compiler_params=params_of,
        name="regroup",
    )(arrived)
    return pl.pallas_call(
        functools.partial(update, pick, window, devices // rows),
        out_shape=(
            jax.ShapeDtypeStruct(momentum.shape, jnp.float32),
            jax.ShapeDtypeStruct(params.shape, jnp.float32),
        ),
        in_specs=[vmem] * 4,
        out_specs=(vmem, vmem),
        scratch_shapes=[pltpu.VMEM((block, PAIR * devices), jnp.float32)],
        compiler_params=params_of,
        name="update",
    )(grouped.reshape(tiles + 1, PAIR * devices, block), slot_map, momentum, params)


def solution(mesh):
    placed = (
        P(("grp", "blk"), None, None),
        P(("grp", "blk"), None),
        P(("grp", "blk"), None),
        P(("grp", "blk"), None),
        P(("grp", "blk"), None),
    )
    return jax.shard_map(
        shards,
        mesh=mesh,
        in_specs=placed,
        out_specs=(P(("grp", "blk"), None), P(("grp", "blk"), None)),
        check_vma=False,
    )
```

```python
import functools

import jax
import jax.numpy as jnp
from jax import lax
from jax.experimental import pallas as pl
from jax.experimental.pallas import tpu as pltpu
from jax.sharding import PartitionSpec as P

PAIR = 2
VMEM_LIMIT = 16 * 1024 * 1024


def pack(owners, tiles, window, grads_ref, picks_ref, out_ref, numbers_ref, sems):
    read = pltpu.make_async_copy(picks_ref, numbers_ref, sems.at[0])
    copy = pltpu.make_async_copy(grads_ref, out_ref.at[:, 0:tiles], sems.at[1])
    read.start()
    copy.start()
    read.wait()
    rows = numbers_ref.shape[0]
    share = owners // rows
    offsets = lax.rem(numbers_ref[...], window).astype(jnp.float32).astype(jnp.bfloat16)
    for r in range(rows):
        row = jnp.broadcast_to(offsets[r : r + 1][None], (share, PAIR, offsets.shape[1]))
        out_ref[r * share : (r + 1) * share, tiles] = row
    copy.wait()


def regroup(tiles, got_ref, slots_ref, out_ref, placing_ref, sems):
    copies = [pltpu.make_async_copy(got_ref.at[:, k], out_ref.at[k], sems.at[k]) for k in range(tiles + 1)]
    for copy in copies:
        copy.start()
    numbered = lax.broadcasted_iota(jnp.int32, placing_ref.shape, 0)
    placing_ref[...] = jnp.where(numbered == slots_ref[...], 1.0, 0.0).astype(jnp.bfloat16)
    for copy in copies:
        copy.wait()


def update(pick, window, share, got, placing, mom, par, new_mom, new_par, numbers):
    tiles = pick // PAIR
    owned, block = mom.shape
    count = got.shape[1]
    first = lax.rem(lax.axis_index("blk"), share) * pick
    numbers[...] = got[tiles].astype(jnp.float32).T
    mine = numbers[pl.ds(pl.multiple_of(first, pick), pick), :]
    lane = lax.broadcasted_iota(jnp.int32, (1, count), 1)
    odd = lax.rem(lane, PAIR) == 1
    place = lax.broadcasted_iota(jnp.int32, (PAIR * window, count), 0).astype(jnp.float32)
    parts = []
    for k in range(tiles):
        key = jnp.where(odd, mine[PAIR * k + 1 : PAIR * k + 2] + float(window), mine[PAIR * k : PAIR * k + 1])
        onehot = jnp.where(place == key, 1.0, 0.0).astype(jnp.bfloat16)
        parts.append(jnp.dot(onehot, got[k], preferred_element_type=jnp.float32))
    merged = jnp.concatenate(parts, axis=0)
    high = merged.astype(jnp.bfloat16)
    rest = merged - high.astype(jnp.float32)
    middle = rest.astype(jnp.bfloat16)
    low = (rest - middle.astype(jnp.float32)).astype(jnp.bfloat16)
    pieces = jnp.concatenate([high, middle, low], axis=1)
    sums = jnp.dot(placing[...], pieces, preferred_element_type=jnp.float32)
    gradient = sums[:, :block] + (sums[:, block : 2 * block] + sums[:, 2 * block :])
    new_momentum = 0.9 * mom[...] + gradient
    new_mom[...] = new_momentum
    new_par[...] = par[...] - 0.05 * (gradient + 0.9 * new_momentum)


def shards(grads, picks, slot_map, momentum, params):
    devices = lax.axis_size("grp") * lax.axis_size("blk")
    items, block = grads.shape[1:]
    owned = slot_map.shape[1]
    pick = items // devices
    tiles = pick // PAIR
    window = owned // pick
    rows = items // block
    vmem = pl.BlockSpec(memory_space=pltpu.VMEM)
    distant = pl.BlockSpec(memory_space=pltpu.HBM)
    in_hbm = functools.partial(pltpu.with_memory_space_constraint, memory_space=pltpu.HBM)
    limits = pltpu.CompilerParams(vmem_limit_bytes=VMEM_LIMIT)
    packed = pl.pallas_call(
        functools.partial(pack, devices, tiles, window),
        out_shape=jax.ShapeDtypeStruct((devices, tiles + 1, PAIR, block), grads.dtype),
        in_specs=[distant, distant],
        out_specs=vmem,
        scratch_shapes=[pltpu.VMEM((rows, block), jnp.int32), pltpu.SemaphoreType.DMA((2,))],
        compiler_params=limits,
        name="pack",
    )(in_hbm(grads.reshape(devices, tiles, PAIR, block)), in_hbm(picks.reshape(rows, block)))
    arrived = lax.all_to_all(packed, ("grp", "blk"), split_axis=0, concat_axis=0, tiled=True)
    grouped, placing = pl.pallas_call(
        functools.partial(regroup, tiles),
        out_shape=(
            jax.ShapeDtypeStruct((tiles + 1, devices, PAIR, block), grads.dtype),
            jax.ShapeDtypeStruct((owned, owned), jnp.bfloat16),
        ),
        in_specs=[vmem, vmem],
        out_specs=(vmem, vmem),
        scratch_shapes=[pltpu.SemaphoreType.DMA((tiles + 1,))],
        compiler_params=limits,
        name="regroup",
    )(arrived, slot_map)
    return pl.pallas_call(
        functools.partial(update, pick, window, devices // rows),
        out_shape=(
            jax.ShapeDtypeStruct(momentum.shape, jnp.float32),
            jax.ShapeDtypeStruct(params.shape, jnp.float32),
        ),
        in_specs=[vmem] * 4,
        out_specs=(vmem, vmem),
        scratch_shapes=[
            pltpu.VMEM((block, PAIR * devices), jnp.float32),
        ],
        compiler_params=limits,
        name="update",
    )(grouped.reshape(tiles + 1, PAIR * devices, block), placing, momentum, params)


def solution(mesh):
    placed = (
        P(("grp", "blk"), None, None),
        P(("grp", "blk"), None),
        P(("grp", "blk"), None),
        P(("grp", "blk"), None),
        P(("grp", "blk"), None),
    )
    return jax.shard_map(
        shards,
        mesh=mesh,
        in_specs=placed,
        out_specs=(P(("grp", "blk"), None), P(("grp", "blk"), None)),
        check_vma=False,
    )
```

```python
import functools

import jax
import jax.numpy as jnp
from jax import lax
from jax.experimental import pallas as pl
from jax.experimental.pallas import tpu as pltpu
from jax.sharding import PartitionSpec as P

PAIR = 2
VMEM_LIMIT = 16 * 1024 * 1024


def pack(tiles, window, grads_ref, picks_ref, out_ref, numbers_ref, sems):
    read = pltpu.make_async_copy(picks_ref, numbers_ref, sems.at[PAIR])
    copies = [
        pltpu.make_async_copy(
            grads_ref.at[:, side], out_ref.at[:, :, side * tiles : (side + 1) * tiles], sems.at[side]
        )
        for side in range(PAIR)
    ]
    read.start()
    for copy in copies:
        copy.start()
    read.wait()
    groups, columns = out_ref.shape[:2]
    rows = numbers_ref.shape[0] // (PAIR * groups)
    share = columns // rows
    offsets = lax.rem(numbers_ref[...], window).astype(jnp.float32)
    for g in range(groups):
        for r in range(rows):
            at = [(g * PAIR + side) * rows + r for side in range(PAIR)]
            two = jnp.concatenate([offsets[a : a + 1] for a in at], axis=0).astype(jnp.bfloat16)
            out_ref[g, r * share : (r + 1) * share, PAIR * tiles] = jnp.broadcast_to(
                two[None], (share,) + two.shape
            )
    for copy in copies:
        copy.wait()


def side_of(mine):
    core = lax.rem(lax.axis_index("grp"), PAIR)
    return core if mine else 1 - core


def regroup_theirs(tiles, got_ref, out_ref, sems):
    start = side_of(False) * tiles
    at = [start + k for k in range(tiles)] + [PAIR * tiles]
    copies = [pltpu.make_async_copy(got_ref.at[:, t], out_ref.at[k], sems.at[k]) for k, t in enumerate(at)]
    for copy in copies:
        copy.start()
    for copy in copies:
        copy.wait()


def regroup_mine(tiles, got_ref, slots_ref, out_ref, placing_ref, sems):
    start = side_of(True) * tiles
    copies = [pltpu.make_async_copy(got_ref.at[:, start + k], out_ref.at[k], sems.at[k]) for k in range(tiles)]
    for copy in copies:
        copy.start()
    numbered = lax.broadcasted_iota(jnp.int32, placing_ref.shape, 0)
    placing_ref[...] = jnp.where(numbered == slots_ref[...], 1.0, 0.0).astype(jnp.bfloat16)
    for copy in copies:
        copy.wait()


def add_up(mine, pick, window, share, got, theirs, sums, numbers):
    tiles = pick // PAIR
    count = got.shape[1]
    side = side_of(mine)
    numbers[...] = theirs[tiles].astype(jnp.float32).T
    first = lax.rem(lax.axis_index("blk"), share) * pick
    both = numbers[pl.ds(pl.multiple_of(first, pick), pick), :]
    odd = lax.rem(lax.broadcasted_iota(jnp.int32, (1, count), 1), PAIR)
    beside = jnp.where(side == 0, pltpu.roll(both, 1, 1), pltpu.roll(both, count - 1, 1))
    chosen = jnp.where(odd == side, both, beside)
    place = lax.broadcasted_iota(jnp.int32, (PAIR * window, count), 0).astype(jnp.float32)
    for k in range(tiles):
        key = jnp.where(odd == 1, chosen[PAIR * k + 1 : PAIR * k + 2] + float(window), chosen[PAIR * k : PAIR * k + 1])
        onehot = jnp.where(place == key, 1.0, 0.0).astype(jnp.bfloat16)
        sums[PAIR * window * k : PAIR * window * (k + 1)] = jnp.dot(
            onehot, got[k], preferred_element_type=jnp.float32
        )


def update(here, there, placing, mom, par, new_mom, new_par):
    block = mom.shape[1]
    merged = here[...] + there[...]
    high = merged.astype(jnp.bfloat16)
    rest = merged - high.astype(jnp.float32)
    middle = rest.astype(jnp.bfloat16)
    low = (rest - middle.astype(jnp.float32)).astype(jnp.bfloat16)
    pieces = jnp.concatenate([high, middle, low], axis=1)
    sums = jnp.dot(placing[...], pieces, preferred_element_type=jnp.float32)
    gradient = sums[:, :block] + (sums[:, block : 2 * block] + sums[:, 2 * block :])
    new_momentum = 0.9 * mom[...] + gradient
    new_mom[...] = new_momentum
    new_par[...] = par[...] - 0.05 * (gradient + 0.9 * new_momentum)


def shards(grads, picks, slot_map, momentum, params):
    groups, columns = lax.axis_size("grp"), lax.axis_size("blk")
    items, block = grads.shape[1:]
    owned = slot_map.shape[1]
    pick = items // (groups * columns)
    tiles = pick // PAIR
    window = owned // pick
    share = block // pick
    pairs = groups // PAIR
    sources = pairs * columns
    vmem = pl.BlockSpec(memory_space=pltpu.VMEM)
    distant = pl.BlockSpec(memory_space=pltpu.HBM)
    in_hbm = functools.partial(pltpu.with_memory_space_constraint, memory_space=pltpu.HBM)
    limits = pltpu.CompilerParams(vmem_limit_bytes=VMEM_LIMIT)
    packed = pl.pallas_call(
        functools.partial(pack, tiles, window),
        out_shape=jax.ShapeDtypeStruct((pairs, columns, PAIR * tiles + 1, PAIR, block), grads.dtype),
        in_specs=[distant, distant],
        out_specs=vmem,
        scratch_shapes=[pltpu.VMEM((items // block, block), jnp.int32), pltpu.SemaphoreType.DMA((PAIR + 1,))],
        compiler_params=limits,
        name="pack",
    )(
        in_hbm(grads.reshape(pairs, PAIR, columns, tiles, PAIR, block)),
        in_hbm(picks.reshape(items // block, block)),
    )
    arrived = lax.all_to_all(
        packed.reshape(sources, PAIR * tiles + 1, PAIR, block),
        ("grp", "blk"),
        split_axis=0,
        concat_axis=0,
        tiled=True,
        axis_index_groups=[
            [(g * PAIR + side) * columns + b for g in range(pairs) for b in range(columns)]
            for side in range(PAIR)
        ],
    )

    def summed(mine, values, theirs):
        return pl.pallas_call(
            functools.partial(add_up, mine, pick, window, share),
            out_shape=jax.ShapeDtypeStruct(momentum.shape, jnp.float32),
            in_specs=[vmem, vmem],
            out_specs=vmem,
            scratch_shapes=[pltpu.VMEM((block, PAIR * sources), jnp.float32)],
            compiler_params=limits,
            cost_estimate=pl.CostEstimate(
                flops=2 * owned * PAIR * sources * block, bytes_accessed=items * block * 2, transcendentals=0
            ),
            name="sum_mine" if mine else "sum_theirs",
        )(values, theirs)

    theirs = pl.pallas_call(
        functools.partial(regroup_theirs, tiles),
        out_shape=jax.ShapeDtypeStruct((tiles + 1, sources, PAIR, block), grads.dtype),
        in_specs=[vmem],
        out_specs=vmem,
        scratch_shapes=[pltpu.SemaphoreType.DMA((tiles + 1,))],
        compiler_params=limits,
        name="regroup_theirs",
    )(arrived).reshape(tiles + 1, PAIR * sources, block)
    there = lax.ppermute(summed(False, theirs, theirs), "grp", [(g, g ^ 1) for g in range(groups)])
    ours, placing = pl.pallas_call(
        functools.partial(regroup_mine, tiles),
        out_shape=(
            jax.ShapeDtypeStruct((tiles, sources, PAIR, block), grads.dtype),
            jax.ShapeDtypeStruct((owned, owned), jnp.bfloat16),
        ),
        in_specs=[vmem, vmem],
        out_specs=(vmem, vmem),
        scratch_shapes=[pltpu.SemaphoreType.DMA((tiles,))],
        compiler_params=limits,
        cost_estimate=pl.CostEstimate(flops=owned * owned * block, bytes_accessed=items * block * 2, transcendentals=0),
        name="regroup_mine",
    )(arrived, slot_map)
    here = summed(True, ours.reshape(tiles, PAIR * sources, block), theirs)
    return pl.pallas_call(
        update,
        out_shape=(
            jax.ShapeDtypeStruct(momentum.shape, jnp.float32),
            jax.ShapeDtypeStruct(params.shape, jnp.float32),
        ),
        in_specs=[vmem] * 5,
        out_specs=(vmem, vmem),
        compiler_params=limits,
        name="update",
    )(here, there, placing, momentum, params)


def solution(mesh):
    placed = (
        P(("grp", "blk"), None, None),
        P(("grp", "blk"), None),
        P(("grp", "blk"), None),
        P(("grp", "blk"), None),
        P(("grp", "blk"), None),
    )
    return jax.shard_map(
        shards,
        mesh=mesh,
        in_specs=placed,
        out_specs=(P(("grp", "blk"), None), P(("grp", "blk"), None)),
        check_vma=False,
    )
```

```python
import functools

import jax
import jax.numpy as jnp
from jax import lax
from jax.experimental import pallas as pl
from jax.experimental.pallas import tpu as pltpu
from jax.sharding import PartitionSpec as P

PAIR = 2
VMEM_LIMIT = 16 * 1024 * 1024


def pack(tiles, window, grads_ref, picks_ref, out_ref, numbers_ref, sems):
    read = pltpu.make_async_copy(picks_ref, numbers_ref, sems.at[PAIR])
    copies = [
        pltpu.make_async_copy(
            grads_ref.at[:, side], out_ref.at[:, :, side * tiles : (side + 1) * tiles], sems.at[side]
        )
        for side in range(PAIR)
    ]
    read.start()
    for copy in copies:
        copy.start()
    read.wait()
    groups, columns = out_ref.shape[:2]
    rows = numbers_ref.shape[0] // (PAIR * groups)
    share = columns // rows
    offsets = lax.rem(numbers_ref[...], window).astype(jnp.float32)
    for g in range(groups):
        for r in range(rows):
            at = [(g * PAIR + side) * rows + r for side in range(PAIR)]
            two = jnp.concatenate([offsets[a : a + 1] for a in at], axis=0).astype(jnp.bfloat16)
            out_ref[g, r * share : (r + 1) * share, PAIR * tiles] = jnp.broadcast_to(
                two[None], (share,) + two.shape
            )
    for copy in copies:
        copy.wait()


def side_of(mine):
    core = lax.rem(lax.axis_index("grp"), PAIR)
    return core if mine else 1 - core


def regroup_theirs(tiles, got_ref, out_ref, sems):
    start = side_of(False) * tiles
    at = [start + k for k in range(tiles)] + [PAIR * tiles]
    copies = [pltpu.make_async_copy(got_ref.at[:, t], out_ref.at[k], sems.at[k]) for k, t in enumerate(at)]
    for copy in copies:
        copy.start()
    for copy in copies:
        copy.wait()


def regroup_mine(tiles, got_ref, slots_ref, out_ref, placing_ref, sems):
    start = side_of(True) * tiles
    copies = [pltpu.make_async_copy(got_ref.at[:, start + k], out_ref.at[k], sems.at[k]) for k in range(tiles)]
    for copy in copies:
        copy.start()
    numbered = lax.broadcasted_iota(jnp.int32, placing_ref.shape, 0)
    placing_ref[...] = jnp.where(numbered == slots_ref[...], 1.0, 0.0).astype(jnp.bfloat16)
    for copy in copies:
        copy.wait()


def add_up(mine, pick, window, share, got, theirs, sums, numbers):
    tiles = pick // PAIR
    count = got.shape[1]
    side = side_of(mine)
    numbers[...] = theirs[tiles].astype(jnp.float32).T
    first = lax.rem(lax.axis_index("blk"), share) * pick
    both = numbers[pl.ds(pl.multiple_of(first, pick), pick), :]
    odd = lax.rem(lax.broadcasted_iota(jnp.int32, (1, count), 1), PAIR)
    beside = jnp.where(side == 0, pltpu.roll(both, 1, 1), pltpu.roll(both, count - 1, 1))
    chosen = jnp.where(odd == side, both, beside)
    place = lax.broadcasted_iota(jnp.int32, (PAIR * window, count), 0).astype(jnp.float32)
    for k in range(tiles):
        key = jnp.where(odd == 1, chosen[PAIR * k + 1 : PAIR * k + 2] + float(window), chosen[PAIR * k : PAIR * k + 1])
        onehot = jnp.where(place == key, 1.0, 0.0).astype(jnp.bfloat16)
        sums[PAIR * window * k : PAIR * window * (k + 1)] = jnp.dot(
            onehot, got[k], preferred_element_type=jnp.float32
        )


def update(here, there, placing, mom, par, new_mom, new_par):
    block = mom.shape[1]
    merged = here[...] + there[...]
    high = merged.astype(jnp.bfloat16)
    rest = merged - high.astype(jnp.float32)
    middle = rest.astype(jnp.bfloat16)
    low = (rest - middle.astype(jnp.float32)).astype(jnp.bfloat16)
    pieces = jnp.concatenate([high, middle, low], axis=1)
    sums = jnp.dot(placing[...], pieces, preferred_element_type=jnp.float32)
    gradient = sums[:, :block] + (sums[:, block : 2 * block] + sums[:, 2 * block :])
    new_momentum = 0.9 * mom[...] + gradient
    new_mom[...] = new_momentum
    new_par[...] = par[...] - 0.05 * (gradient + 0.9 * new_momentum)


def shards(grads, picks, slot_map, momentum, params):
    groups, columns = lax.axis_size("grp"), lax.axis_size("blk")
    items, block = grads.shape[1:]
    owned = slot_map.shape[1]
    pick = items // (groups * columns)
    tiles = pick // PAIR
    window = owned // pick
    share = block // pick
    pairs = groups // PAIR
    sources = pairs * columns
    vmem = pl.BlockSpec(memory_space=pltpu.VMEM)
    distant = pl.BlockSpec(memory_space=pltpu.HBM)
    in_hbm = functools.partial(pltpu.with_memory_space_constraint, memory_space=pltpu.HBM)
    limits = pltpu.CompilerParams(vmem_limit_bytes=VMEM_LIMIT)
    packed = pl.pallas_call(
        functools.partial(pack, tiles, window),
        out_shape=jax.ShapeDtypeStruct((pairs, columns, PAIR * tiles + 1, PAIR, block), grads.dtype),
        in_specs=[distant, distant],
        out_specs=vmem,
        scratch_shapes=[pltpu.VMEM((items // block, block), jnp.int32), pltpu.SemaphoreType.DMA((PAIR + 1,))],
        compiler_params=limits,
        name="pack",
    )(
        in_hbm(grads.reshape(pairs, PAIR, columns, tiles, PAIR, block)),
        in_hbm(picks.reshape(items // block, block)),
    )
    arrived = lax.all_to_all(
        packed.reshape(sources, PAIR * tiles + 1, PAIR, block),
        ("grp", "blk"),
        split_axis=0,
        concat_axis=0,
        tiled=True,
        axis_index_groups=[
            [(g * PAIR + (g + b + side) % PAIR) * columns + b for g in range(pairs) for b in range(columns)]
            for side in range(PAIR)
        ],
    )

    def summed(mine, values, theirs):
        return pl.pallas_call(
            functools.partial(add_up, mine, pick, window, share),
            out_shape=jax.ShapeDtypeStruct(momentum.shape, jnp.float32),
            in_specs=[vmem, vmem],
            out_specs=vmem,
            scratch_shapes=[pltpu.VMEM((block, PAIR * sources), jnp.float32)],
            compiler_params=limits,
            cost_estimate=pl.CostEstimate(
                flops=2 * owned * PAIR * sources * block, bytes_accessed=items * block * 2, transcendentals=0
            ),
            name="sum_mine" if mine else "sum_theirs",
        )(values, theirs)

    theirs = pl.pallas_call(
        functools.partial(regroup_theirs, tiles),
        out_shape=jax.ShapeDtypeStruct((tiles + 1, sources, PAIR, block), grads.dtype),
        in_specs=[vmem],
        out_specs=vmem,
        scratch_shapes=[pltpu.SemaphoreType.DMA((tiles + 1,))],
        compiler_params=limits,
        name="regroup_theirs",
    )(arrived).reshape(tiles + 1, PAIR * sources, block)
    there = lax.ppermute(summed(False, theirs, theirs), "grp", [(g, g ^ 1) for g in range(groups)])
    ours, placing = pl.pallas_call(
        functools.partial(regroup_mine, tiles),
        out_shape=(
            jax.ShapeDtypeStruct((tiles, sources, PAIR, block), grads.dtype),
            jax.ShapeDtypeStruct((owned, owned), jnp.bfloat16),
        ),
        in_specs=[vmem, vmem],
        out_specs=(vmem, vmem),
        scratch_shapes=[pltpu.SemaphoreType.DMA((tiles,))],
        compiler_params=limits,
        cost_estimate=pl.CostEstimate(flops=owned * owned * block, bytes_accessed=items * block * 2, transcendentals=0),
        name="regroup_mine",
    )(arrived, slot_map)
    here = summed(True, ours.reshape(tiles, PAIR * sources, block), theirs)
    return pl.pallas_call(
        update,
        out_shape=(
            jax.ShapeDtypeStruct(momentum.shape, jnp.float32),
            jax.ShapeDtypeStruct(params.shape, jnp.float32),
        ),
        in_specs=[vmem] * 5,
        out_specs=(vmem, vmem),
        compiler_params=limits,
        name="update",
    )(here, there, placing, momentum, params)


def solution(mesh):
    placed = (
        P(("grp", "blk"), None, None),
        P(("grp", "blk"), None),
        P(("grp", "blk"), None),
        P(("grp", "blk"), None),
        P(("grp", "blk"), None),
    )
    return jax.shard_map(
        shards,
        mesh=mesh,
        in_specs=placed,
        out_specs=(P(("grp", "blk"), None), P(("grp", "blk"), None)),
        check_vma=False,
    )
```

```python
import functools

import jax
import jax.numpy as jnp
from jax import lax
from jax.experimental import pallas as pl
from jax.experimental.pallas import tpu as pltpu
from jax.sharding import PartitionSpec as P

PAIR = 2
VMEM_LIMIT = 16 * 1024 * 1024


def pack(tiles, window, grads_ref, picks_ref, out_ref, numbers_ref, sems):
    read = pltpu.make_async_copy(picks_ref, numbers_ref, sems.at[PAIR])
    copies = [
        pltpu.make_async_copy(
            grads_ref.at[:, side], out_ref.at[:, :, side * tiles : (side + 1) * tiles], sems.at[side]
        )
        for side in range(PAIR)
    ]
    read.start()
    for copy in copies:
        copy.start()
    read.wait()
    groups, columns = out_ref.shape[:2]
    rows = numbers_ref.shape[0] // (PAIR * groups)
    share = columns // rows
    offsets = lax.rem(numbers_ref[...], window).astype(jnp.float32)
    for g in range(groups):
        for r in range(rows):
            at = [(g * PAIR + side) * rows + r for side in range(PAIR)]
            two = jnp.concatenate([offsets[a : a + 1] for a in at], axis=0).astype(jnp.bfloat16)
            out_ref[g, r * share : (r + 1) * share, PAIR * tiles] = jnp.broadcast_to(
                two[None], (share,) + two.shape
            )
    for copy in copies:
        copy.wait()


def side_of():
    return lax.rem(lax.axis_index("grp"), PAIR)


def regroup(got_ref, slots_ref, out_ref, placing_ref, sems):
    copies = [
        pltpu.make_async_copy(got_ref.at[:, k], out_ref.at[k], sems.at[k]) for k in range(out_ref.shape[0])
    ]
    for copy in copies:
        copy.start()
    numbered = lax.broadcasted_iota(jnp.int32, placing_ref.shape, 0)
    placing_ref[...] = jnp.where(numbered == slots_ref[...], 1.0, 0.0).astype(jnp.bfloat16)
    for copy in copies:
        copy.wait()


def add_up(pick, window, share, got, here, there, numbers):
    tiles = pick // PAIR
    count = got.shape[1]
    numbers[...] = got[PAIR * tiles].astype(jnp.float32).T
    first = lax.rem(lax.axis_index("blk"), share) * pick
    both = numbers[pl.ds(pl.multiple_of(first, pick), pick), :]
    odd = lax.rem(lax.broadcasted_iota(jnp.int32, (1, count), 1), PAIR)
    place = lax.broadcasted_iota(jnp.int32, (PAIR * window, count), 0).astype(jnp.float32)
    core = side_of()
    beside = (pltpu.roll(both, 1, 1), pltpu.roll(both, count - 1, 1))
    for side, sums in ((1 - core, there), (core, here)):
        chosen = jnp.where(odd == side, both, jnp.where(side == 0, beside[0], beside[1]))
        for k in range(tiles):
            key = jnp.where(
                odd == 1, chosen[PAIR * k + 1 : PAIR * k + 2] + float(window), chosen[PAIR * k : PAIR * k + 1]
            )
            onehot = jnp.where(place == key, 1.0, 0.0).astype(jnp.bfloat16)
            sums[PAIR * window * k : PAIR * window * (k + 1)] = jnp.dot(
                onehot, got[side * tiles + k], preferred_element_type=jnp.float32
            )


def update(here, swapped, placing, mom, par, new_mom, new_par):
    owned, block = mom.shape
    other = pl.multiple_of((1 - side_of()) * owned, owned)
    merged = here[...] + swapped[pl.ds(other, owned), :]
    high = merged.astype(jnp.bfloat16)
    rest = merged - high.astype(jnp.float32)
    pieces = jnp.concatenate([high, rest.astype(jnp.bfloat16)], axis=1)
    sums = jnp.dot(placing[...], pieces, preferred_element_type=jnp.float32)
    gradient = sums[:, :block] + sums[:, block:]
    new_momentum = 0.9 * mom[...] + gradient
    new_mom[...] = new_momentum
    new_par[...] = par[...] - 0.05 * (gradient + 0.9 * new_momentum)


def shards(grads, picks, slot_map, momentum, params):
    groups, columns = lax.axis_size("grp"), lax.axis_size("blk")
    items, block = grads.shape[1:]
    owned = slot_map.shape[1]
    pick = items // (groups * columns)
    tiles = pick // PAIR
    window = owned // pick
    share = block // pick
    pairs = groups // PAIR
    sources = pairs * columns
    vmem = pl.BlockSpec(memory_space=pltpu.VMEM)
    distant = pl.BlockSpec(memory_space=pltpu.HBM)
    in_hbm = functools.partial(pltpu.with_memory_space_constraint, memory_space=pltpu.HBM)
    limits = pltpu.CompilerParams(vmem_limit_bytes=VMEM_LIMIT)
    packed = pl.pallas_call(
        functools.partial(pack, tiles, window),
        out_shape=jax.ShapeDtypeStruct((pairs, columns, PAIR * tiles + 1, PAIR, block), grads.dtype),
        in_specs=[distant, distant],
        out_specs=vmem,
        scratch_shapes=[pltpu.VMEM((items // block, block), jnp.int32), pltpu.SemaphoreType.DMA((PAIR + 1,))],
        compiler_params=limits,
        name="pack",
    )(
        in_hbm(grads.reshape(pairs, PAIR, columns, tiles, PAIR, block)),
        in_hbm(picks.reshape(items // block, block)),
    )
    arrived = lax.all_to_all(
        packed.reshape(sources, PAIR * tiles + 1, PAIR, block),
        ("grp", "blk"),
        split_axis=0,
        concat_axis=0,
        tiled=True,
        axis_index_groups=[
            [(g * PAIR + (g + b + side) % PAIR) * columns + b for g in range(pairs) for b in range(columns)]
            for side in range(PAIR)
        ],
    )

    grouped, placing = pl.pallas_call(
        regroup,
        out_shape=(
            jax.ShapeDtypeStruct((PAIR * tiles + 1, sources, PAIR, block), grads.dtype),
            jax.ShapeDtypeStruct((owned, owned), jnp.bfloat16),
        ),
        in_specs=[vmem, vmem],
        out_specs=(vmem, vmem),
        scratch_shapes=[pltpu.SemaphoreType.DMA((PAIR * tiles + 1,))],
        compiler_params=limits,
        name="regroup",
    )(arrived, slot_map)
    here, there = pl.pallas_call(
        functools.partial(add_up, pick, window, share),
        out_shape=(jax.ShapeDtypeStruct(momentum.shape, jnp.float32),) * 2,
        in_specs=[vmem],
        out_specs=(vmem, vmem),
        scratch_shapes=[pltpu.VMEM((block, PAIR * sources), jnp.float32)],
        compiler_params=limits,
        name="add_up",
    )(grouped.reshape(PAIR * tiles + 1, PAIR * sources, block))
    swapped = lax.all_gather(
        there,
        "grp",
        axis_index_groups=[[g, g + 1] for g in range(0, groups, PAIR)],
        tiled=True,
    )
    return pl.pallas_call(
        update,
        out_shape=(
            jax.ShapeDtypeStruct(momentum.shape, jnp.float32),
            jax.ShapeDtypeStruct(params.shape, jnp.float32),
        ),
        in_specs=[vmem] * 5,
        out_specs=(vmem, vmem),
        compiler_params=limits,
        name="update",
    )(here, swapped, placing, momentum, params)


def solution(mesh):
    placed = (
        P(("grp", "blk"), None, None),
        P(("grp", "blk"), None),
        P(("grp", "blk"), None),
        P(("grp", "blk"), None),
        P(("grp", "blk"), None),
    )
    return jax.shard_map(
        shards,
        mesh=mesh,
        in_specs=placed,
        out_specs=(P(("grp", "blk"), None), P(("grp", "blk"), None)),
        check_vma=False,
    )
```

```python
import functools

import jax
import jax.numpy as jnp
from jax import lax
from jax.experimental import pallas as pl
from jax.experimental.pallas import tpu as pltpu
from jax.sharding import PartitionSpec as P

PAIR = 2
VMEM_LIMIT = 16 * 1024 * 1024


def pack(tiles, window, grads_ref, picks_ref, out_ref, numbers_ref, sems):
    read = pltpu.make_async_copy(picks_ref, numbers_ref, sems.at[PAIR])
    copies = [
        pltpu.make_async_copy(
            grads_ref.at[:, side], out_ref.at[:, :, side * tiles : (side + 1) * tiles], sems.at[side]
        )
        for side in range(PAIR)
    ]
    read.start()
    for copy in copies:
        copy.start()
    read.wait()
    groups, columns = out_ref.shape[:2]
    rows = numbers_ref.shape[0] // (PAIR * groups)
    share = columns // rows
    offsets = lax.rem(numbers_ref[...], window).astype(jnp.float32)
    for g in range(groups):
        for r in range(rows):
            at = [(g * PAIR + side) * rows + r for side in range(PAIR)]
            two = jnp.concatenate([offsets[a : a + 1] for a in at], axis=0).astype(jnp.bfloat16)
            out_ref[g, r * share : (r + 1) * share, PAIR * tiles] = jnp.broadcast_to(
                two[None], (share,) + two.shape
            )
    for copy in copies:
        copy.wait()


def side_of():
    return lax.rem(lax.axis_index("grp"), PAIR)


def add_up(pick, window, share, got, slots, here, there, placing, numbers):
    tiles = pick // PAIR
    count = got.shape[1]
    numbers[...] = got[PAIR * tiles].astype(jnp.float32).T
    first = lax.rem(lax.axis_index("blk"), share) * pick
    both = numbers[pl.ds(pl.multiple_of(first, pick), pick), :]
    numbered = lax.broadcasted_iota(jnp.int32, placing.shape, 0)
    placing[...] = jnp.where(numbered == slots[...], 1.0, 0.0).astype(jnp.bfloat16)
    odd = lax.rem(lax.broadcasted_iota(jnp.int32, (1, count), 1), PAIR)
    place = lax.broadcasted_iota(jnp.int32, (PAIR * window, count), 0).astype(jnp.float32)
    core = side_of()
    beside = (pltpu.roll(both, 1, 1), pltpu.roll(both, count - 1, 1))
    for side, sums in ((1 - core, there), (core, here)):
        chosen = jnp.where(odd == side, both, jnp.where(side == 0, beside[0], beside[1]))
        for k in range(tiles):
            key = jnp.where(
                odd == 1, chosen[PAIR * k + 1 : PAIR * k + 2] + float(window), chosen[PAIR * k : PAIR * k + 1]
            )
            onehot = jnp.where(place == key, 1.0, 0.0).astype(jnp.bfloat16)
            sums[PAIR * window * k : PAIR * window * (k + 1)] = jnp.dot(
                onehot, got[side * tiles + k], preferred_element_type=jnp.float32
            )


def update(here, swapped, placing, mom, par, new_mom, new_par):
    owned, block = mom.shape
    other = pl.multiple_of((1 - side_of()) * owned, owned)
    merged = here[...] + swapped[pl.ds(other, owned), :]
    high = merged.astype(jnp.bfloat16)
    rest = merged - high.astype(jnp.float32)
    pieces = jnp.concatenate([high, rest.astype(jnp.bfloat16)], axis=1)
    sums = jnp.dot(placing[...], pieces, preferred_element_type=jnp.float32)
    gradient = sums[:, :block] + sums[:, block:]
    new_momentum = 0.9 * mom[...] + gradient
    new_mom[...] = new_momentum
    new_par[...] = par[...] - 0.05 * (gradient + 0.9 * new_momentum)


def shards(grads, picks, slot_map, momentum, params):
    groups, columns = lax.axis_size("grp"), lax.axis_size("blk")
    items, block = grads.shape[1:]
    owned = slot_map.shape[1]
    pick = items // (groups * columns)
    tiles = pick // PAIR
    window = owned // pick
    share = block // pick
    pairs = groups // PAIR
    sources = pairs * columns
    vmem = pl.BlockSpec(memory_space=pltpu.VMEM)
    distant = pl.BlockSpec(memory_space=pltpu.HBM)
    in_hbm = functools.partial(pltpu.with_memory_space_constraint, memory_space=pltpu.HBM)
    limits = pltpu.CompilerParams(vmem_limit_bytes=VMEM_LIMIT)
    packed = pl.pallas_call(
        functools.partial(pack, tiles, window),
        out_shape=jax.ShapeDtypeStruct((pairs, columns, PAIR * tiles + 1, PAIR, block), grads.dtype),
        in_specs=[distant, distant],
        out_specs=vmem,
        scratch_shapes=[pltpu.VMEM((items // block, block), jnp.int32), pltpu.SemaphoreType.DMA((PAIR + 1,))],
        compiler_params=limits,
        name="pack",
    )(
        in_hbm(grads.reshape(pairs, PAIR, columns, tiles, PAIR, block)),
        in_hbm(picks.reshape(items // block, block)),
    )
    arrived = lax.all_to_all(
        packed.reshape(sources, PAIR * tiles + 1, PAIR, block),
        ("grp", "blk"),
        split_axis=0,
        concat_axis=0,
        tiled=True,
        axis_index_groups=[
            [(g * PAIR + (g + b + side) % PAIR) * columns + b for g in range(pairs) for b in range(columns)]
            for side in range(PAIR)
        ],
    )

    grouped = jnp.swapaxes(arrived, 0, 1).reshape(PAIR * tiles + 1, PAIR * sources, block)
    here, there, placing = pl.pallas_call(
        functools.partial(add_up, pick, window, share),
        out_shape=(
            jax.ShapeDtypeStruct(momentum.shape, jnp.float32),
            jax.ShapeDtypeStruct(momentum.shape, jnp.float32),
            jax.ShapeDtypeStruct((owned, owned), jnp.bfloat16),
        ),
        in_specs=[vmem, vmem],
        out_specs=(vmem, vmem, vmem),
        scratch_shapes=[pltpu.VMEM((block, PAIR * sources), jnp.float32)],
        compiler_params=limits,
        name="add_up",
    )(grouped, slot_map)
    swapped = lax.all_gather(
        there,
        "grp",
        axis_index_groups=[[g, g + 1] for g in range(0, groups, PAIR)],
        tiled=True,
    )
    return pl.pallas_call(
        update,
        out_shape=(
            jax.ShapeDtypeStruct(momentum.shape, jnp.float32),
            jax.ShapeDtypeStruct(params.shape, jnp.float32),
        ),
        in_specs=[vmem] * 5,
        out_specs=(vmem, vmem),
        compiler_params=limits,
        name="update",
    )(here, swapped, placing, momentum, params)


def solution(mesh):
    placed = (
        P(("grp", "blk"), None, None),
        P(("grp", "blk"), None),
        P(("grp", "blk"), None),
        P(("grp", "blk"), None),
        P(("grp", "blk"), None),
    )
    return jax.shard_map(
        shards,
        mesh=mesh,
        in_specs=placed,
        out_specs=(P(("grp", "blk"), None), P(("grp", "blk"), None)),
        check_vma=False,
    )
```

```python
import functools

import jax
import jax.numpy as jnp
from jax import lax
from jax.experimental import pallas as pl
from jax.experimental.pallas import tpu as pltpu
from jax.sharding import PartitionSpec as P

PAIR = 2
VMEM_LIMIT = 16 * 1024 * 1024


def pack(tiles, window, grads_ref, picks_ref, out_ref, numbers_ref, sems):
    read = pltpu.make_async_copy(picks_ref, numbers_ref, sems.at[PAIR])
    copies = [
        pltpu.make_async_copy(
            grads_ref.at[:, side], out_ref.at[:, :, side * tiles : (side + 1) * tiles], sems.at[side]
        )
        for side in range(PAIR)
    ]
    read.start()
    for copy in copies:
        copy.start()
    read.wait()
    groups, columns = out_ref.shape[:2]
    rows = numbers_ref.shape[0] // (PAIR * groups)
    share = columns // rows
    offsets = lax.rem(numbers_ref[...], window).astype(jnp.float32)
    for g in range(groups):
        for r in range(rows):
            at = [(g * PAIR + side) * rows + r for side in range(PAIR)]
            two = jnp.concatenate([offsets[a : a + 1] for a in at], axis=0).astype(jnp.bfloat16)
            out_ref[g, r * share : (r + 1) * share, PAIR * tiles] = jnp.broadcast_to(
                two[None], (share,) + two.shape
            )
    for copy in copies:
        copy.wait()


def side_of():
    return lax.rem(lax.axis_index("grp"), PAIR)


def place(slots, placing):
    numbered = lax.broadcasted_iota(jnp.int32, placing.shape, 0)
    placing[...] = jnp.where(numbered == slots[...], 1.0, 0.0).astype(jnp.bfloat16)


def add_up(pick, window, share, got, here, there, numbers):
    tiles = pick // PAIR
    count = got.shape[1]
    numbers[...] = got[PAIR * tiles].astype(jnp.float32).T
    first = lax.rem(lax.axis_index("blk"), share) * pick
    both = numbers[pl.ds(pl.multiple_of(first, pick), pick), :]
    odd = lax.rem(lax.broadcasted_iota(jnp.int32, (1, count), 1), PAIR)
    place = lax.broadcasted_iota(jnp.int32, (PAIR * window, count), 0).astype(jnp.float32)
    core = side_of()
    beside = (pltpu.roll(both, 1, 1), pltpu.roll(both, count - 1, 1))
    for side, sums in ((1 - core, there), (core, here)):
        chosen = jnp.where(odd == side, both, jnp.where(side == 0, beside[0], beside[1]))
        for k in range(tiles):
            key = jnp.where(
                odd == 1, chosen[PAIR * k + 1 : PAIR * k + 2] + float(window), chosen[PAIR * k : PAIR * k + 1]
            )
            onehot = jnp.where(place == key, 1.0, 0.0).astype(jnp.bfloat16)
            sums[PAIR * window * k : PAIR * window * (k + 1)] = jnp.dot(
                onehot, got[side * tiles + k], preferred_element_type=jnp.float32
            )


def update(here, swapped, placing, mom, par, new_mom, new_par):
    owned, block = mom.shape
    other = pl.multiple_of((1 - side_of()) * owned, owned)
    merged = here[...] + swapped[pl.ds(other, owned), :]
    high = merged.astype(jnp.bfloat16)
    rest = merged - high.astype(jnp.float32)
    pieces = jnp.concatenate([high, rest.astype(jnp.bfloat16)], axis=1)
    sums = jnp.dot(placing[...], pieces, preferred_element_type=jnp.float32)
    gradient = sums[:, :block] + sums[:, block:]
    new_momentum = 0.9 * mom[...] + gradient
    new_mom[...] = new_momentum
    new_par[...] = par[...] - 0.05 * (gradient + 0.9 * new_momentum)


def shards(grads, picks, slot_map, momentum, params):
    groups, columns = lax.axis_size("grp"), lax.axis_size("blk")
    items, block = grads.shape[1:]
    owned = slot_map.shape[1]
    pick = items // (groups * columns)
    tiles = pick // PAIR
    window = owned // pick
    share = block // pick
    pairs = groups // PAIR
    sources = pairs * columns
    vmem = pl.BlockSpec(memory_space=pltpu.VMEM)
    distant = pl.BlockSpec(memory_space=pltpu.HBM)
    in_hbm = functools.partial(pltpu.with_memory_space_constraint, memory_space=pltpu.HBM)
    limits = pltpu.CompilerParams(vmem_limit_bytes=VMEM_LIMIT)
    packed = pl.pallas_call(
        functools.partial(pack, tiles, window),
        out_shape=jax.ShapeDtypeStruct((pairs, columns, PAIR * tiles + 1, PAIR, block), grads.dtype),
        in_specs=[distant, distant],
        out_specs=vmem,
        scratch_shapes=[pltpu.VMEM((items // block, block), jnp.int32), pltpu.SemaphoreType.DMA((PAIR + 1,))],
        compiler_params=limits,
        name="pack",
    )(
        in_hbm(grads.reshape(pairs, PAIR, columns, tiles, PAIR, block)),
        in_hbm(picks.reshape(items // block, block)),
    )
    arrived = lax.all_to_all(
        packed.reshape(sources, PAIR * tiles + 1, PAIR, block),
        ("grp", "blk"),
        split_axis=0,
        concat_axis=0,
        tiled=True,
        axis_index_groups=[
            [(g * PAIR + (g + b + side) % PAIR) * columns + b for g in range(pairs) for b in range(columns)]
            for side in range(PAIR)
        ],
    )
    placing = pl.pallas_call(
        place,
        out_shape=jax.ShapeDtypeStruct((owned, owned), jnp.bfloat16),
        in_specs=[vmem],
        out_specs=vmem,
        compiler_params=limits,
        name="place",
    )(slot_map)

    grouped = jnp.swapaxes(arrived, 0, 1).reshape(PAIR * tiles + 1, PAIR * sources, block)
    here, there = pl.pallas_call(
        functools.partial(add_up, pick, window, share),
        out_shape=(
            jax.ShapeDtypeStruct(momentum.shape, jnp.float32),
            jax.ShapeDtypeStruct(momentum.shape, jnp.float32),
        ),
        in_specs=[vmem],
        out_specs=(vmem, vmem),
        scratch_shapes=[pltpu.VMEM((block, PAIR * sources), jnp.float32)],
        compiler_params=limits,
        name="add_up",
    )(grouped)
    swapped = lax.all_gather(
        there,
        "grp",
        axis_index_groups=[[g, g + 1] for g in range(0, groups, PAIR)],
        tiled=True,
    )
    return pl.pallas_call(
        update,
        out_shape=(
            jax.ShapeDtypeStruct(momentum.shape, jnp.float32),
            jax.ShapeDtypeStruct(params.shape, jnp.float32),
        ),
        in_specs=[vmem] * 5,
        out_specs=(vmem, vmem),
        compiler_params=limits,
        name="update",
    )(here, swapped, placing, momentum, params)


def solution(mesh):
    placed = (
        P(("grp", "blk"), None, None),
        P(("grp", "blk"), None),
        P(("grp", "blk"), None),
        P(("grp", "blk"), None),
        P(("grp", "blk"), None),
    )
    return jax.shard_map(
        shards,
        mesh=mesh,
        in_specs=placed,
        out_specs=(P(("grp", "blk"), None), P(("grp", "blk"), None)),
        check_vma=False,
    )
```

```python
import functools

import jax
import jax.numpy as jnp
from jax import lax
from jax.experimental import pallas as pl
from jax.experimental.pallas import tpu as pltpu
from jax.sharding import PartitionSpec as P

PAIR = 2
ALONG_X = 4
VMEM_LIMIT = 16 * 1024 * 1024


def pack(tiles, window, grads_ref, picks_ref, out_ref, numbers_ref, sems):
    read = pltpu.make_async_copy(picks_ref, numbers_ref, sems.at[PAIR])
    copies = [
        pltpu.make_async_copy(
            grads_ref.at[:, side], out_ref.at[:, :, side * tiles : (side + 1) * tiles], sems.at[side]
        )
        for side in range(PAIR)
    ]
    read.start()
    for copy in copies:
        copy.start()
    read.wait()
    groups, columns = out_ref.shape[:2]
    rows = numbers_ref.shape[0] // (PAIR * groups)
    share = columns // rows
    offsets = lax.rem(numbers_ref[...], window).astype(jnp.float32)
    for g in range(groups):
        for r in range(rows):
            at = [(g * PAIR + side) * rows + r for side in range(PAIR)]
            two = jnp.concatenate([offsets[a : a + 1] for a in at], axis=0).astype(jnp.bfloat16)
            out_ref[g, r * share : (r + 1) * share, PAIR * tiles] = jnp.broadcast_to(
                two[None], (share,) + two.shape
            )
    for copy in copies:
        copy.wait()


def side_of():
    return lax.rem(lax.axis_index("grp"), PAIR)


def add_up(pick, window, share, got, slots, here, there, placing, numbers):
    tiles = pick // PAIR
    count = got.shape[1]
    numbers[...] = got[PAIR * tiles].astype(jnp.float32).T
    first = lax.rem(lax.axis_index("blk"), share) * pick
    both = numbers[pl.ds(pl.multiple_of(first, pick), pick), :]
    numbered = lax.broadcasted_iota(jnp.int32, placing.shape, 0)
    placing[...] = jnp.where(numbered == slots[...], 1.0, 0.0).astype(jnp.bfloat16)
    odd = lax.rem(lax.broadcasted_iota(jnp.int32, (1, count), 1), PAIR)
    place = lax.broadcasted_iota(jnp.int32, (PAIR * window, count), 0).astype(jnp.float32)
    core = side_of()
    beside = (pltpu.roll(both, 1, 1), pltpu.roll(both, count - 1, 1))
    for side, sums in ((1 - core, there), (core, here)):
        chosen = jnp.where(odd == side, both, jnp.where(side == 0, beside[0], beside[1]))
        for k in range(tiles):
            key = jnp.where(
                odd == 1, chosen[PAIR * k + 1 : PAIR * k + 2] + float(window), chosen[PAIR * k : PAIR * k + 1]
            )
            onehot = jnp.where(place == key, 1.0, 0.0).astype(jnp.bfloat16)
            sums[PAIR * window * k : PAIR * window * (k + 1)] = jnp.dot(
                onehot, got[side * tiles + k], preferred_element_type=jnp.float32
            )


def update(here, swapped, placing, mom, par, new_mom, new_par):
    owned, block = mom.shape
    other = pl.multiple_of((1 - side_of()) * owned, owned)
    merged = here[...] + swapped[pl.ds(other, owned), :]
    high = merged.astype(jnp.bfloat16)
    rest = merged - high.astype(jnp.float32)
    pieces = jnp.concatenate([high, rest.astype(jnp.bfloat16)], axis=1)
    sums = jnp.dot(placing[...], pieces, preferred_element_type=jnp.float32)
    gradient = sums[:, :block] + sums[:, block:]
    new_momentum = 0.9 * mom[...] + gradient
    new_mom[...] = new_momentum
    new_par[...] = par[...] - 0.05 * (gradient + 0.9 * new_momentum)


def shards(grads, picks, slot_map, momentum, params):
    groups, columns = lax.axis_size("grp"), lax.axis_size("blk")
    items, block = grads.shape[1:]
    owned = slot_map.shape[1]
    pick = items // (groups * columns)
    tiles = pick // PAIR
    window = owned // pick
    share = block // pick
    pairs = groups // PAIR
    sources = pairs * columns
    vmem = pl.BlockSpec(memory_space=pltpu.VMEM)
    distant = pl.BlockSpec(memory_space=pltpu.HBM)
    in_hbm = functools.partial(pltpu.with_memory_space_constraint, memory_space=pltpu.HBM)
    limits = pltpu.CompilerParams(vmem_limit_bytes=VMEM_LIMIT)
    packed = pl.pallas_call(
        functools.partial(pack, tiles, window),
        out_shape=jax.ShapeDtypeStruct((pairs, columns, PAIR * tiles + 1, PAIR, block), grads.dtype),
        in_specs=[distant, distant],
        out_specs=vmem,
        scratch_shapes=[pltpu.VMEM((items // block, block), jnp.int32), pltpu.SemaphoreType.DMA((PAIR + 1,))],
        compiler_params=limits,
        name="pack",
    )(
        in_hbm(grads.reshape(pairs, PAIR, columns, tiles, PAIR, block)),
        in_hbm(picks.reshape(items // block, block)),
    )
    arrived = lax.all_to_all(
        packed.reshape(sources, PAIR * tiles + 1, PAIR, block),
        ("grp", "blk"),
        split_axis=0,
        concat_axis=0,
        tiled=True,
        axis_index_groups=[
            [
                (g * PAIR + (g + b // ALONG_X + b % ALONG_X + side) % PAIR) * columns + b
                for g in range(pairs)
                for b in range(columns)
            ]
            for side in range(PAIR)
        ],
    )

    grouped = jnp.swapaxes(arrived, 0, 1).reshape(PAIR * tiles + 1, PAIR * sources, block)
    here, there, placing = pl.pallas_call(
        functools.partial(add_up, pick, window, share),
        out_shape=(
            jax.ShapeDtypeStruct(momentum.shape, jnp.float32),
            jax.ShapeDtypeStruct(momentum.shape, jnp.float32),
            jax.ShapeDtypeStruct((owned, owned), jnp.bfloat16),
        ),
        in_specs=[vmem, vmem],
        out_specs=(vmem, vmem, vmem),
        scratch_shapes=[pltpu.VMEM((block, PAIR * sources), jnp.float32)],
        compiler_params=limits,
        name="add_up",
    )(grouped, slot_map)
    swapped = lax.all_gather(
        there,
        "grp",
        axis_index_groups=[[g, g + 1] for g in range(0, groups, PAIR)],
        tiled=True,
    )
    return pl.pallas_call(
        update,
        out_shape=(
            jax.ShapeDtypeStruct(momentum.shape, jnp.float32),
            jax.ShapeDtypeStruct(params.shape, jnp.float32),
        ),
        in_specs=[vmem] * 5,
        out_specs=(vmem, vmem),
        compiler_params=limits,
        name="update",
    )(here, swapped, placing, momentum, params)


def solution(mesh):
    placed = (
        P(("grp", "blk"), None, None),
        P(("grp", "blk"), None),
        P(("grp", "blk"), None),
        P(("grp", "blk"), None),
        P(("grp", "blk"), None),
    )
    return jax.shard_map(
        shards,
        mesh=mesh,
        in_specs=placed,
        out_specs=(P(("grp", "blk"), None), P(("grp", "blk"), None)),
        check_vma=False,
    )
```

```python
import functools

import jax
import jax.numpy as jnp
from jax import lax
from jax.experimental import pallas as pl
from jax.experimental.pallas import tpu as pltpu
from jax.sharding import PartitionSpec as P

PAIR = 2
VMEM_LIMIT = 16 * 1024 * 1024


def pack(tiles, window, grads_ref, picks_ref, out_ref, numbers_ref, sems):
    groups, columns = out_ref.shape[:2]
    at = lax.axis_index("grp")
    group = lax.rem(lax.rem(at, PAIR) + at // PAIR + lax.axis_index("blk"), PAIR)
    spots = [jnp.where(group == 0, g, groups - 1 - g) for g in range(groups)]
    read = pltpu.make_async_copy(picks_ref, numbers_ref, sems.at[PAIR * groups])
    copies = [
        pltpu.make_async_copy(
            grads_ref.at[g, side],
            out_ref.at[spots[g], :, side * tiles : (side + 1) * tiles],
            sems.at[g * PAIR + side],
        )
        for g in range(groups)
        for side in range(PAIR)
    ]
    read.start()
    for copy in copies:
        copy.start()
    read.wait()
    rows = numbers_ref.shape[0] // (PAIR * groups)
    share = columns // rows
    offsets = lax.rem(numbers_ref[...], window).astype(jnp.float32)
    for g in range(groups):
        for r in range(rows):
            lines = [(g * PAIR + side) * rows + r for side in range(PAIR)]
            two = jnp.concatenate([offsets[a : a + 1] for a in lines], axis=0).astype(jnp.bfloat16)
            out_ref[spots[g], r * share : (r + 1) * share, PAIR * tiles] = jnp.broadcast_to(
                two[None], (share,) + two.shape
            )
    for copy in copies:
        copy.wait()


def side_of():
    return lax.rem(lax.axis_index("grp"), PAIR)


def add_up(pick, window, share, got, slots, here, there, placing, numbers):
    tiles = pick // PAIR
    count = got.shape[1]
    numbers[...] = got[PAIR * tiles].astype(jnp.float32).T
    first = lax.rem(lax.axis_index("blk"), share) * pick
    both = numbers[pl.ds(pl.multiple_of(first, pick), pick), :]
    numbered = lax.broadcasted_iota(jnp.int32, placing.shape, 0)
    placing[...] = jnp.where(numbered == slots[...], 1.0, 0.0).astype(jnp.bfloat16)
    odd = lax.rem(lax.broadcasted_iota(jnp.int32, (1, count), 1), PAIR)
    place = lax.broadcasted_iota(jnp.int32, (PAIR * window, count), 0).astype(jnp.float32)
    core = side_of()
    beside = (pltpu.roll(both, 1, 1), pltpu.roll(both, count - 1, 1))
    for side, sums in ((1 - core, there), (core, here)):
        chosen = jnp.where(odd == side, both, jnp.where(side == 0, beside[0], beside[1]))
        for k in range(tiles):
            key = jnp.where(
                odd == 1, chosen[PAIR * k + 1 : PAIR * k + 2] + float(window), chosen[PAIR * k : PAIR * k + 1]
            )
            onehot = jnp.where(place == key, 1.0, 0.0).astype(jnp.bfloat16)
            sums[PAIR * window * k : PAIR * window * (k + 1)] = jnp.dot(
                onehot, got[side * tiles + k], preferred_element_type=jnp.float32
            )


def update(here, swapped, placing, mom, par, new_mom, new_par):
    owned, block = mom.shape
    other = pl.multiple_of((1 - side_of()) * owned, owned)
    merged = here[...] + swapped[pl.ds(other, owned), :]
    high = merged.astype(jnp.bfloat16)
    rest = merged - high.astype(jnp.float32)
    pieces = jnp.concatenate([high, rest.astype(jnp.bfloat16)], axis=1)
    sums = jnp.dot(placing[...], pieces, preferred_element_type=jnp.float32)
    gradient = sums[:, :block] + sums[:, block:]
    new_momentum = 0.9 * mom[...] + gradient
    new_mom[...] = new_momentum
    new_par[...] = par[...] - 0.05 * (gradient + 0.9 * new_momentum)


def shards(grads, picks, slot_map, momentum, params):
    groups, columns = lax.axis_size("grp"), lax.axis_size("blk")
    items, block = grads.shape[1:]
    owned = slot_map.shape[1]
    pick = items // (groups * columns)
    tiles = pick // PAIR
    window = owned // pick
    share = block // pick
    pairs = groups // PAIR
    sources = pairs * columns
    vmem = pl.BlockSpec(memory_space=pltpu.VMEM)
    distant = pl.BlockSpec(memory_space=pltpu.HBM)
    in_hbm = functools.partial(pltpu.with_memory_space_constraint, memory_space=pltpu.HBM)
    limits = pltpu.CompilerParams(vmem_limit_bytes=VMEM_LIMIT)
    packed = pl.pallas_call(
        functools.partial(pack, tiles, window),
        out_shape=jax.ShapeDtypeStruct((pairs, columns, PAIR * tiles + 1, PAIR, block), grads.dtype),
        in_specs=[distant, distant],
        out_specs=vmem,
        scratch_shapes=[pltpu.VMEM((items // block, block), jnp.int32), pltpu.SemaphoreType.DMA((items // (columns * pick) + 1,))],
        compiler_params=limits,
        name="pack",
    )(
        in_hbm(grads.reshape(pairs, PAIR, columns, tiles, PAIR, block)),
        in_hbm(picks.reshape(items // block, block)),
    )
    arrived = lax.all_to_all(
        packed.reshape(sources, PAIR * tiles + 1, PAIR, block),
        ("grp", "blk"),
        split_axis=0,
        concat_axis=0,
        tiled=True,
        axis_index_groups=[
            [
                (g * PAIR + (g + b + side) % PAIR) * columns + b
                for g in (reversed(range(pairs)) if side else range(pairs))
                for b in range(columns)
            ]
            for side in range(PAIR)
        ],
    )

    grouped = jnp.swapaxes(arrived, 0, 1).reshape(PAIR * tiles + 1, PAIR * sources, block)
    here, there, placing = pl.pallas_call(
        functools.partial(add_up, pick, window, share),
        out_shape=(
            jax.ShapeDtypeStruct(momentum.shape, jnp.float32),
            jax.ShapeDtypeStruct(momentum.shape, jnp.float32),
            jax.ShapeDtypeStruct((owned, owned), jnp.bfloat16),
        ),
        in_specs=[vmem, vmem],
        out_specs=(vmem, vmem, vmem),
        scratch_shapes=[pltpu.VMEM((block, PAIR * sources), jnp.float32)],
        compiler_params=limits,
        name="add_up",
    )(grouped, slot_map)
    swapped = lax.all_gather(
        there,
        "grp",
        axis_index_groups=[[g, g + 1] for g in range(0, groups, PAIR)],
        tiled=True,
    )
    return pl.pallas_call(
        update,
        out_shape=(
            jax.ShapeDtypeStruct(momentum.shape, jnp.float32),
            jax.ShapeDtypeStruct(params.shape, jnp.float32),
        ),
        in_specs=[vmem] * 5,
        out_specs=(vmem, vmem),
        compiler_params=limits,
        name="update",
    )(here, swapped, placing, momentum, params)


def solution(mesh):
    placed = (
        P(("grp", "blk"), None, None),
        P(("grp", "blk"), None),
        P(("grp", "blk"), None),
        P(("grp", "blk"), None),
        P(("grp", "blk"), None),
    )
    return jax.shard_map(
        shards,
        mesh=mesh,
        in_specs=placed,
        out_specs=(P(("grp", "blk"), None), P(("grp", "blk"), None)),
        check_vma=False,
    )
```

```python
import functools

import jax
import jax.numpy as jnp
from jax import lax
from jax.experimental import pallas as pl
from jax.experimental.pallas import tpu as pltpu
from jax.sharding import PartitionSpec as P

PAIR = 2
VMEM_LIMIT = 16 * 1024 * 1024


def places(count):
    listed = [i // 2 if i % 2 == 0 else count - 1 - i // 2 for i in range(count)]
    return [listed.index(i) for i in range(count)]


def pack(tiles, window, grads_ref, picks_ref, out_ref, numbers_ref, sems):
    groups, columns = out_ref.shape[:2]
    at = lax.axis_index("grp")
    group = lax.rem(lax.rem(at, PAIR) + at // PAIR + lax.axis_index("blk"), PAIR)
    spots = [jnp.where(group == 0, p, groups - 1 - p) for p in places(groups)]
    read = pltpu.make_async_copy(picks_ref, numbers_ref, sems.at[PAIR * groups])
    copies = [
        pltpu.make_async_copy(
            grads_ref.at[g, side],
            out_ref.at[spots[g], :, side * tiles : (side + 1) * tiles],
            sems.at[g * PAIR + side],
        )
        for g in range(groups)
        for side in range(PAIR)
    ]
    read.start()
    for copy in copies:
        copy.start()
    read.wait()
    rows = numbers_ref.shape[0] // (PAIR * groups)
    share = columns // rows
    offsets = lax.rem(numbers_ref[...], window).astype(jnp.float32)
    for g in range(groups):
        for r in range(rows):
            lines = [(g * PAIR + side) * rows + r for side in range(PAIR)]
            two = jnp.concatenate([offsets[a : a + 1] for a in lines], axis=0).astype(jnp.bfloat16)
            out_ref[spots[g], r * share : (r + 1) * share, PAIR * tiles] = jnp.broadcast_to(
                two[None], (share,) + two.shape
            )
    for copy in copies:
        copy.wait()


def side_of():
    return lax.rem(lax.axis_index("grp"), PAIR)


def add_up(pick, window, share, got, slots, here, there, placing, numbers):
    tiles = pick // PAIR
    count = got.shape[1]
    numbers[...] = got[PAIR * tiles].astype(jnp.float32).T
    first = lax.rem(lax.axis_index("blk"), share) * pick
    both = numbers[pl.ds(pl.multiple_of(first, pick), pick), :]
    numbered = lax.broadcasted_iota(jnp.int32, placing.shape, 0)
    placing[...] = jnp.where(numbered == slots[...], 1.0, 0.0).astype(jnp.bfloat16)
    odd = lax.rem(lax.broadcasted_iota(jnp.int32, (1, count), 1), PAIR)
    place = lax.broadcasted_iota(jnp.int32, (PAIR * window, count), 0).astype(jnp.float32)
    core = side_of()
    beside = (pltpu.roll(both, 1, 1), pltpu.roll(both, count - 1, 1))
    for side, sums in ((1 - core, there), (core, here)):
        chosen = jnp.where(odd == side, both, jnp.where(side == 0, beside[0], beside[1]))
        for k in range(tiles):
            key = jnp.where(
                odd == 1, chosen[PAIR * k + 1 : PAIR * k + 2] + float(window), chosen[PAIR * k : PAIR * k + 1]
            )
            onehot = jnp.where(place == key, 1.0, 0.0).astype(jnp.bfloat16)
            sums[PAIR * window * k : PAIR * window * (k + 1)] = jnp.dot(
                onehot, got[side * tiles + k], preferred_element_type=jnp.float32
            )


def update(here, swapped, placing, mom, par, new_mom, new_par):
    owned, block = mom.shape
    other = pl.multiple_of((1 - side_of()) * owned, owned)
    merged = here[...] + swapped[pl.ds(other, owned), :]
    high = merged.astype(jnp.bfloat16)
    rest = merged - high.astype(jnp.float32)
    pieces = jnp.concatenate([high, rest.astype(jnp.bfloat16)], axis=1)
    sums = jnp.dot(placing[...], pieces, preferred_element_type=jnp.float32)
    gradient = sums[:, :block] + sums[:, block:]
    new_momentum = 0.9 * mom[...] + gradient
    new_mom[...] = new_momentum
    new_par[...] = par[...] - 0.05 * (gradient + 0.9 * new_momentum)


def shards(grads, picks, slot_map, momentum, params):
    groups, columns = lax.axis_size("grp"), lax.axis_size("blk")
    items, block = grads.shape[1:]
    owned = slot_map.shape[1]
    pick = items // (groups * columns)
    tiles = pick // PAIR
    window = owned // pick
    share = block // pick
    pairs = groups // PAIR
    sources = pairs * columns
    vmem = pl.BlockSpec(memory_space=pltpu.VMEM)
    distant = pl.BlockSpec(memory_space=pltpu.HBM)
    in_hbm = functools.partial(pltpu.with_memory_space_constraint, memory_space=pltpu.HBM)
    limits = pltpu.CompilerParams(vmem_limit_bytes=VMEM_LIMIT)
    packed = pl.pallas_call(
        functools.partial(pack, tiles, window),
        out_shape=jax.ShapeDtypeStruct((pairs, columns, PAIR * tiles + 1, PAIR, block), grads.dtype),
        in_specs=[distant, distant],
        out_specs=vmem,
        scratch_shapes=[pltpu.VMEM((items // block, block), jnp.int32), pltpu.SemaphoreType.DMA((items // (columns * pick) + 1,))],
        compiler_params=limits,
        name="pack",
    )(
        in_hbm(grads.reshape(pairs, PAIR, columns, tiles, PAIR, block)),
        in_hbm(picks.reshape(items // block, block)),
    )
    arrived = lax.all_to_all(
        packed.reshape(sources, PAIR * tiles + 1, PAIR, block),
        ("grp", "blk"),
        split_axis=0,
        concat_axis=0,
        tiled=True,
        axis_index_groups=[
            [
                (g * PAIR + (g + b + side) % PAIR) * columns + b
                for g in sorted(range(pairs), key=places(pairs).__getitem__, reverse=bool(side))
                for b in range(columns)
            ]
            for side in range(PAIR)
        ],
    )

    grouped = jnp.swapaxes(arrived, 0, 1).reshape(PAIR * tiles + 1, PAIR * sources, block)
    here, there, placing = pl.pallas_call(
        functools.partial(add_up, pick, window, share),
        out_shape=(
            jax.ShapeDtypeStruct(momentum.shape, jnp.float32),
            jax.ShapeDtypeStruct(momentum.shape, jnp.float32),
            jax.ShapeDtypeStruct((owned, owned), jnp.bfloat16),
        ),
        in_specs=[vmem, vmem],
        out_specs=(vmem, vmem, vmem),
        scratch_shapes=[pltpu.VMEM((block, PAIR * sources), jnp.float32)],
        compiler_params=limits,
        name="add_up",
    )(grouped, slot_map)
    swapped = lax.all_gather(
        there,
        "grp",
        axis_index_groups=[[g, g + 1] for g in range(0, groups, PAIR)],
        tiled=True,
    )
    return pl.pallas_call(
        update,
        out_shape=(
            jax.ShapeDtypeStruct(momentum.shape, jnp.float32),
            jax.ShapeDtypeStruct(params.shape, jnp.float32),
        ),
        in_specs=[vmem] * 5,
        out_specs=(vmem, vmem),
        compiler_params=limits,
        name="update",
    )(here, swapped, placing, momentum, params)


def solution(mesh):
    placed = (
        P(("grp", "blk"), None, None),
        P(("grp", "blk"), None),
        P(("grp", "blk"), None),
        P(("grp", "blk"), None),
        P(("grp", "blk"), None),
    )
    return jax.shard_map(
        shards,
        mesh=mesh,
        in_specs=placed,
        out_specs=(P(("grp", "blk"), None), P(("grp", "blk"), None)),
        check_vma=False,
    )
```
